512 devices in a mesh: rows: 32 (over x, z_lo), cols: 16 (over z_hi, y, core).
Axes of the slice: x: 4, y: 4, z: 16 (z_hi: 2, z_lo: 8; z = z_hi * 8 + z_lo), core: 2. Of those that a mesh axis runs over, the one named last changes fastest.
Arguments:
- image_in: bfloat16 [1, 512, 1536, 256], P(None, 'rows', 'cols'), may hold values from -6 to 6
- cotangent: bfloat16 [1, 512, 1536, 256], P(None, 'rows', 'cols'), may hold values from -6 to 6
- first_kernel: bfloat16 [3, 3, 256, 256], replicated, may hold values from -0.125 to 0.125
- first_bias: float32 [256], replicated, may hold values from -3 to 3
- second_kernel: bfloat16 [3, 3, 256, 256], replicated, may hold values from -0.125 to 0.125
- first_center: float32 [32], replicated, may hold values from -3 to 3
- first_inverse: float32 [32], replicated, may hold values from 0.5 to 2
- first_gain: float32 [256], replicated, may hold values from 0.5 to 1.5
- first_shift: float32 [256], replicated, may hold values from -3 to 3
- second_center: float32 [32], replicated, may hold values from -3 to 3
- second_inverse: float32 [32], replicated, may hold values from 0.5 to 2
- second_gain: float32 [256], replicated, may hold values from 0.5 to 1.5
- second_shift: float32 [256], replicated, may hold values from -3 to 3
Outputs:
- image_grad: bfloat16 [1, 512, 1536, 256], P(None, 'rows', 'cols')
The draws below stay inside these ranges and needn't reach their ends.
All inputs are finite; a program needn't handle non-finite values.
Results may differ from the reference program's by a relative error of at most 0.0044.
Values may be sent and summed in bfloat16 or wider, within the bound.
No kernel may reach another device: no remote copies, remote signals or barrier semaphores. Data moves between devices by JAX's collectives and lax.ppermute only.
A program may use at most 64 MiB of HBM per device.

```python
import math
import jax
import jax.numpy as jnp
from jax import lax

CHANNELS = 256
GROUPS = 32
IMAGES = 1
HEIGHT = 512
WIDTH = 1536


def block_levels(key, shape, pieces, least, largest):
    loudness, own = 1.0, jax.random.fold_in(key, 6)
    for dim, shards_of in pieces:
        draws = jnp.exp(jax.random.uniform(jax.random.fold_in(own, dim), (shards_of,), jnp.float32, least / len(pieces), largest / len(pieces)))
        loudness = loudness * jnp.repeat(draws, shape[dim] // shards_of).reshape([-1 if axis == dim else 1 for axis in range(len(shape))])
    return loudness


def noise(stream_key, shape, spread, reach, cuts=(), kind=jnp.bfloat16):
    drawn = spread * jax.random.normal(stream_key, shape, jnp.float32)
    if cuts:
        drawn = drawn * block_levels(stream_key, shape, cuts, -0.22, 0.18)
    return jnp.clip(drawn, -reach, reach).astype(kind)


def setup_inputs(seed: int = 0) -> dict:
    seeds = jax.random.split(jax.random.key(seed), 14)
    return {
        "image_in": noise(seeds[0], (IMAGES, HEIGHT, WIDTH, CHANNELS), 1.0, 6.0, ((1, 32), (2, 16))),
        "cotangent": noise(seeds[1], (IMAGES, HEIGHT, WIDTH, CHANNELS), 1.0, 6.0, ((1, 32), (2, 16))),
        "first_kernel": noise(seeds[2], (3, 3, CHANNELS, CHANNELS), (9 * CHANNELS) ** -0.5, 0.125),
        "first_bias": noise(seeds[3], (CHANNELS,), 0.5, 3.0, (), jnp.float32),
        "second_kernel": noise(seeds[4], (3, 3, CHANNELS, CHANNELS), (9 * CHANNELS) ** -0.5, 0.125),
        "first_center": noise(seeds[5], (GROUPS,), 0.5, 3.0, (), jnp.float32),
        "first_inverse": jnp.clip(jnp.exp(jax.random.uniform(seeds[6], (GROUPS,), jnp.float32, math.log(0.5), math.log(2.0))), 0.5, 2.0),
        "first_gain": jnp.clip(1.0 + 0.1 * jax.random.normal(seeds[7], (CHANNELS,), jnp.float32), 0.5, 1.5),
        "first_shift": noise(seeds[8], (CHANNELS,), 0.5, 3.0, (), jnp.float32),
        "second_center": noise(seeds[9], (GROUPS,), 0.5, 3.0, (), jnp.float32),
        "second_inverse": jnp.clip(jnp.exp(jax.random.uniform(seeds[10], (GROUPS,), jnp.float32, math.log(0.5), math.log(2.0))), 0.5, 2.0),
        "second_gain": jnp.clip(1.0 + 0.1 * jax.random.normal(seeds[11], (CHANNELS,), jnp.float32), 0.5, 1.5),
        "second_shift": noise(seeds[12], (CHANNELS,), 0.5, 3.0, (), jnp.float32),
    }


def per_channel(stat):
    return jnp.repeat(stat, CHANNELS // GROUPS)


def silu_slope(value):
    sig = jax.nn.sigmoid(value)
    return sig * (1.0 + value * (1.0 - sig))


def convolve(field, kernel):
    return lax.conv_general_dilated(field.astype(jnp.float32), kernel.astype(jnp.float32), (1, 1), "SAME", dimension_numbers=("NHWC", "HWIO", "NHWC"), preferred_element_type=jnp.float32)


def flipped(kernel):
    return jnp.transpose(kernel[::-1, ::-1], (0, 1, 3, 2))


def reference(image_in, cotangent, first_kernel, first_bias, second_kernel, first_center, first_inverse, first_gain, first_shift, second_center, second_inverse, second_gain, second_shift):
    scale_one = per_channel(first_inverse) * first_gain
    scale_two = per_channel(second_inverse) * second_gain
    kernel_back_two = flipped(second_kernel)
    kernel_back_one = flipped(first_kernel)

    def one_image(pair):
        image, grad_out = pair
        image = image[None]
        grad_out = grad_out[None]
        pre_one = (image.astype(jnp.float32) - per_channel(first_center)) * scale_one + first_shift
        act_one = jax.nn.silu(pre_one).astype(jnp.bfloat16)
        pre_two = (convolve(act_one, first_kernel) + first_bias - per_channel(second_center)) * scale_two + second_shift
        back_two = convolve(grad_out, kernel_back_two)
        back_inner = (back_two * silu_slope(pre_two) * scale_two).astype(jnp.bfloat16)
        back_one = convolve(back_inner, kernel_back_one)
        result = grad_out.astype(jnp.float32) + back_one * silu_slope(pre_one) * scale_one
        return result.astype(jnp.bfloat16)[0]

    return lax.map(one_image, (image_in, cotangent))
```

```python
import jax
import jax.numpy as jnp
from jax import lax
from jax.experimental import pallas as pl
from jax.experimental.pallas import tpu as pltpu
from jax.sharding import PartitionSpec as P

PADW = 112

def fused_kernel(flags, img, cot, top, bot, left, right, k1, k2, par, out, rowbuf, act3, cot3, in3):
    H, W, C = img.shape[1], img.shape[2], img.shape[3]
    half_one, bias_one = par[0:1, :], par[1:2, :]
    half_two, bias_two, scale_two_h = par[2:3, :], par[3:4, :], par[4:5, :]
    scale_one_h = par[5:6, :]

    def act_of(x):
        h = x.astype(jnp.float32) * half_one + bias_one
        return h * jnp.tanh(h) + h

    def fill(slot, h, own, lft, rgt, dst):
        rb = rowbuf.at[slot]
        rb[2 : 2 + W, :] = own
        rb[0:2, :] = lft
        rb[2 + W : 4 + W, :] = rgt
        for j in range(3):
            dst[j, h, :, :] = rb[j : j + PADW, :].astype(jnp.bfloat16)

    n = 0
    for h in range(H + 4):
        for which, dst in ((0, act3), (1, cot3)):
            if h < 2:
                own = top[which, h]
                m = flags[0]
            elif h >= H + 2:
                own = bot[which, h - H - 2]
                m = flags[1]
            else:
                own = (img if which == 0 else cot)[0, h - 2]
                m = None
            lft, rgt = left[which, h], right[which, h]
            if which == 0:
                own, lft, rgt = act_of(own), act_of(lft) * flags[2], act_of(rgt) * flags[3]
                if m is not None:
                    own, lft, rgt = own * m, lft * m, rgt * m
            else:
                own, lft, rgt = (v.astype(jnp.float32) for v in (own, lft, rgt))
            fill(n % 4, h, own, lft, rgt, dst)
            n += 1

    def conv(src, wref, base, rows, width, flip):
        acc = None
        for i in range(3):
            for j in range(3):
                lhs = src[j, base + i : base + i + rows, 0:width, :].reshape(rows * width, C)
                if flip:
                    t = lax.dot_general(lhs, wref[2 - i, 2 - j], (((1,), (1,)), ((), ())), preferred_element_type=jnp.float32)
                else:
                    t = lax.dot_general(lhs, wref[i, j], (((1,), (0,)), ((), ())), preferred_element_type=jnp.float32)
                acc = t if acc is None else acc + t
        return acc

    R = 6
    pos = lax.broadcasted_iota(jnp.int32, (PADW, 1), 0)
    cmask = jnp.where(pos == 0, flags[2], jnp.where(pos == W + 1, flags[3], 1.0))
    for b in range((H + 2) // R):
        c1 = conv(act3, k1, b * R, R, PADW, False)
        c2 = conv(cot3, k2, b * R, R, PADW, True)
        for r in range(R):
            h = b * R + r
            v = c1[r * PADW : (r + 1) * PADW] * half_two + bias_two
            t = jnp.tanh(v)
            s = (1.0 + t) * (1.0 + v - v * t)
            g = c2[r * PADW : (r + 1) * PADW] * scale_two_h * s * cmask
            if h == 0:
                g = g * flags[0]
            if h == H + 1:
                g = g * flags[1]
            rb = rowbuf.at[h % 4]
            rb[0:PADW, :] = g
            for j in range(3):
                in3[j, h, :, :] = rb[j : j + W, :].astype(jnp.bfloat16)
    R = 8
    for b in range(H // R):
        c3 = conv(in3, k1, b * R, R, W, True)
        for r in range(R):
            h = b * R + r
            v = img[0, h].astype(jnp.float32) * half_one + bias_one
            t = jnp.tanh(v)
            s = (1.0 + t) * (1.0 + v - v * t)
            res = cot[0, h].astype(jnp.float32) + c3[r * W : (r + 1) * W] * scale_one_h * s
            out[0, h] = res.astype(jnp.bfloat16)


def call(flags, img, cot, top, bot, left, right, k1, k2, par):
    H, W, C = img.shape[1:]
    vm = pl.BlockSpec(memory_space=pltpu.VMEM)
    return pl.pallas_call(
        fused_kernel,
        out_shape=jax.ShapeDtypeStruct(img.shape, jnp.bfloat16),
        in_specs=[pl.BlockSpec(memory_space=pltpu.SMEM)] + [vm] * 9,
        out_specs=vm,
        scratch_shapes=[
            pltpu.VMEM((4, PADW + 16, C), jnp.float32),
            pltpu.VMEM((3, H + 4, PADW, C), jnp.bfloat16),
            pltpu.VMEM((3, H + 4, PADW, C), jnp.bfloat16),
            pltpu.VMEM((3, H + 2, W, C), jnp.bfloat16),
        ],
        compiler_params=pltpu.CompilerParams(vmem_limit_bytes=48 << 20),
    )(flags, img, cot, top, bot, left, right, k1, k2, par)


def shifts(axis):
    size = lax.axis_size(axis)
    up = [(i, i + 1) for i in range(size - 1)]
    return up, [(j, i) for i, j in up]


def per_device(
    image_in,
    cotangent,
    first_kernel,
    first_bias,
    second_kernel,
    first_center,
    first_inverse,
    first_gain,
    first_shift,
    second_center,
    second_inverse,
    second_gain,
    second_shift,
):
    tile_cols = image_in.shape[2]
    repeats = image_in.shape[3] // first_center.shape[0]
    center_one = jnp.repeat(first_center, repeats)
    center_two = jnp.repeat(second_center, repeats)
    scale_one = jnp.repeat(first_inverse, repeats) * first_gain
    scale_two = jnp.repeat(second_inverse, repeats) * second_gain
    zero = jnp.zeros_like(scale_one)
    params = jnp.stack(
        (
            0.5 * scale_one,
            0.5 * (first_shift - center_one * scale_one),
            0.5 * scale_two,
            0.5 * ((first_bias - center_two) * scale_two + second_shift),
            0.5 * scale_two,
            0.5 * scale_one,
            zero,
            zero,
        )
    )
    row, col = lax.axis_index("rows"), lax.axis_index("cols")
    flags = jnp.stack(
        (row > 0, row < lax.axis_size("rows") - 1, col > 0, col < lax.axis_size("cols") - 1)
    ).astype(jnp.float32)
    pick = lambda *cut: jnp.concatenate((image_in[cut], cotangent[cut]))
    every = slice(None)
    up, down = shifts("rows")
    top = lax.ppermute(pick(every, slice(-2, None)), "rows", up)
    bottom = lax.ppermute(pick(every, slice(0, 2)), "rows", down)
    up, down = shifts("cols")
    edge = lambda cut: jnp.concatenate((top[:, :, cut], pick(every, every, cut), bottom[:, :, cut]), axis=1)
    left = lax.ppermute(edge(slice(tile_cols - 2, tile_cols)), "cols", up)
    right = lax.ppermute(edge(slice(0, 2)), "cols", down)
    return call(flags, image_in, cotangent, top, bottom, left, right, first_kernel, second_kernel, params)


def solution(mesh):
    tiled, whole = P(None, "rows", "cols", None), P()
    return jax.shard_map(
        per_device,
        mesh=mesh,
        in_specs=(tiled, tiled) + (whole,) * 11,
        out_specs=tiled,
        check_vma=False,
    )
```

```python
import jax
import jax.numpy as jnp
from jax import lax
from jax.experimental import pallas as pl
from jax.experimental.pallas import tpu as pltpu
from jax.sharding import PartitionSpec as P

PADW = 112
F32, BF16 = jnp.float32, jnp.bfloat16
ROWS, COLS = "rows", "cols"
VMEM, HBM, SMEM = (pl.BlockSpec(memory_space=m) for m in (pltpu.VMEM, pltpu.HBM, pltpu.SMEM))
LIMIT = pltpu.CompilerParams(vmem_limit_bytes=40 << 20)


def place():
    row, col = lax.axis_index(ROWS), lax.axis_index(COLS)
    rows, cols = lax.axis_size(ROWS), lax.axis_size(COLS)
    exists = [x.astype(jnp.int32).astype(F32) for x in (row > 0, row < rows - 1, col > 0, col < cols - 1)]
    return row % 2 == 1, col % 2 == 1, exists


def edges_kernel(img, cot, near, far, lo, hi, strip, sems):
    H, W, _ = img.shape[1:]
    copies = []
    for k, x in enumerate((img, cot)):
        copies += [
            pltpu.make_async_copy(x.at[0, :, 0:8, :], lo.at[k], sems.at[2 * k]),
            pltpu.make_async_copy(x.at[0, :, W - 8 : W, :], hi.at[k], sems.at[2 * k + 1]),
        ]
    for c in copies:
        c.start()
    _, odd_col, _ = place()
    for k in range(2):
        copies[2 * k].wait()
        copies[2 * k + 1].wait()
        for h in range(H):
            strip[0, 2 * h : 2 * h + 2, :] = lo[k, h].astype(F32)[0:2]
            strip[1, 2 * h : 2 * h + 2, :] = hi[k, h].astype(F32)[6:8]
        first, last = strip[0].astype(BF16), strip[1].astype(BF16)
        near[k] = jnp.where(odd_col, first, last)
        far[k] = jnp.where(odd_col, last, first)


def edges(img, cot):
    H, _, C = img.shape[1:]
    shape = jax.ShapeDtypeStruct((2, 2 * H, C), BF16)
    return pl.pallas_call(
        edges_kernel,
        out_shape=(shape, shape),
        in_specs=[HBM, HBM],
        out_specs=(VMEM, VMEM),
        scratch_shapes=[
            pltpu.VMEM((2, H, 8, C), BF16),
            pltpu.VMEM((2, H, 8, C), BF16),
            pltpu.VMEM((2, 2 * H, C), F32),
            pltpu.SemaphoreType.DMA((4,)),
        ],
        name="edges",
    )(img, cot)


def messages_kernel(img, cot, ce, co, odd, even, near_own, far_own, buf):
    H, W = img.shape[1], img.shape[2]
    n, m = 2 * W, ce.shape[1]
    odd_row, _, _ = place()
    buf[8:16] = jnp.zeros_like(buf[8:16])
    for k in range(2):
        near_own[k], far_own[k] = ce[k], co[k]
        x = (img, cot)[k]
        for h in range(2):
            upper, lower = x[0, h], x[0, H - 2 + h]
            odd[k, h * W : (h + 1) * W] = jnp.where(odd_row, lower, upper)
            even[k, h * W : (h + 1) * W] = jnp.where(odd_row, upper, lower)
        tops = [r[k, 0:16].astype(F32)[0:4] for r in (ce, co)]
        ends = [r[k, m - 16 : m].astype(F32)[12:16] for r in (ce, co)]
        for dst, flip in ((odd, False), (even, True)):
            for s in range(2):
                first, second = (tops[s], ends[s]) if flip else (ends[s], tops[s])
                buf[4 * s : 4 * s + 4] = jnp.where(odd_row, first, second)
            dst[k, n : n + 16] = buf[...].astype(BF16)


def messages(img, cot, ce, co):
    n, m, C = 2 * img.shape[2], ce.shape[1], ce.shape[2]
    shape = lambda n: jax.ShapeDtypeStruct((2, n, C), BF16)
    return pl.pallas_call(
        messages_kernel,
        out_shape=(shape(n + 16), shape(n + 16), shape(m), shape(m)),
        in_specs=[VMEM] * 4,
        out_specs=(VMEM,) * 4,
        scratch_shapes=[pltpu.VMEM((16, C), F32)],
        name="messages",
    )(img, cot, ce, co)


def per_channel(stat, channels):
    group = lax.broadcasted_iota(jnp.int32, (1, channels), 1) // (channels // stat.shape[0])
    wide = jnp.full((1, channels), stat[0], F32)
    for g in range(1, stat.shape[0]):
        wide = jnp.where(group == g, stat[g], wide)
    return wide


def affine(stats, vecs, C):
    center_one, inverse_one, center_two, inverse_two = (per_channel(v, C) for v in stats)
    bias, gain_one, shift_one, gain_two, shift_two = (v[0:1, :] for v in vecs)
    half_one, half_two = 0.5 * (inverse_one * gain_one), 0.5 * (inverse_two * gain_two)
    bias_one = 0.5 * shift_one - center_one * half_one
    bias_two = (bias - center_two) * half_two + 0.5 * shift_two
    return half_one, bias_one, half_two, bias_two


def act_of(x, half, bias):
    h = x.astype(F32) * half + bias
    return h * jnp.tanh(h) + h


def slope_of(v):
    t = jnp.tanh(v)
    return (1.0 + t) * (1.0 + v - v * t)


def fill(rb, own, lft, rgt, dst, h):
    W = own.shape[0]
    rb[2 : 2 + W, :] = own.astype(F32)
    rb[0:2, :] = lft
    rb[2 + W : 4 + W, :] = rgt
    for j in range(3):
        dst[j, h, :, :] = rb[j : j + PADW, :].astype(BF16)


def conv(src, wref, starts, rows, width, flip):
    C, acc = wref.shape[3], None
    for i in range(3):
        for j in range(3):
            parts = [src[j, b + i : b + i + rows, 0:width, :].reshape(rows * width, C) for b in starts]
            lhs = parts[0] if len(parts) == 1 else jnp.concatenate(parts)
            w = wref[2 - i, 2 - j] if flip else wref[i, j]
            dims = (((1,), (1 if flip else 0,)), ((), ()))
            t = lax.dot_general(lhs, w, dims, preferred_element_type=F32)
            acc = t if acc is None else acc + t
    return acc


def inner_rows(c1, c2, r, half_two, bias_two, cmask):
    cut = slice(r * PADW, (r + 1) * PADW)
    return c2[cut] * half_two * slope_of(c1[cut] * half_two + bias_two) * cmask


def store_inner(rb, g, dst, h, W):
    rb[0:PADW, :] = g
    for j in range(3):
        dst[j, h, :, :] = rb[j : j + W, :].astype(BF16)


def col_mask(to_left, to_right, W):
    pos = lax.broadcasted_iota(jnp.int32, (PADW, 1), 0)
    return jnp.where(pos == 0, to_left, jnp.where(pos == W + 1, to_right, 1.0))


def result_row(x, g, c3, half_one, bias_one):
    v = x.astype(F32) * half_one + bias_one
    return (g.astype(F32) + c3 * half_one * slope_of(v)).astype(BF16)


def middle_kernel(
    stats, vecs, img, cot, ce, co, w1, w2, out, kept, rowbuf, act3, cot3, in3, res, nbuf, fbuf, k1, k2, sems
):
    H, W, C = img.shape[1:]
    loads = [pltpu.make_async_copy(w1, k1, sems.at[0]), pltpu.make_async_copy(w2, k2, sems.at[1])]
    for load in loads:
        load.start()
    half_one, bias_one, half_two, bias_two = affine(stats, vecs, C)
    odd_row, odd_col, (up, down, to_left, to_right) = place()
    for k in range(2):
        nbuf[k], fbuf[k] = ce[k].astype(F32), co[k].astype(F32)
    count = 0
    for h in range(H):
        for k, (src, dst) in enumerate(((img, act3), (cot, cot3))):
            cut = slice(2 * h, 2 * h + 2)
            near, far = nbuf[k, cut], fbuf[k, cut]
            lft, rgt = jnp.where(odd_col, near, far), jnp.where(odd_col, far, near)
            own = src[0, h]
            if k == 0:
                own = act_of(own, half_one, bias_one)
                lft, rgt = act_of(lft, half_one, bias_one) * to_left, act_of(rgt, half_one, bias_one) * to_right
            fill(rowbuf.at[count % 4], own, lft, rgt, dst, h)
            count += 1
    for load in loads:
        load.wait()
    cmask = col_mask(to_left, to_right, W)
    R = (H - 2) // 2
    for b in range(0, H - 2, R):
        c1 = conv(act3, k1, (b,), R, PADW, False)
        c2 = conv(cot3, k2, (b,), R, PADW, True)
        for r in range(R):
            g = inner_rows(c1, c2, r, half_two, bias_two, cmask)
            store_inner(rowbuf.at[r % 4], g, in3, b + r, W)
    for j in range(3):
        for s, h in enumerate((0, 1, H - 4, H - 3)):
            kept[j, s] = in3[j, h]
    R = (H - 4) // 2
    stores = []
    for b in range(0, H - 4, R):
        c3 = conv(in3, k1, (b,), R, W, True)
        for r in range(R):
            h = b + r + 2
            res[b + r] = result_row(img[0, h], cot[0, h], c3[r * W : (r + 1) * W], half_one, bias_one)
        stores.append(pltpu.make_async_copy(res.at[b : b + R], out.at[0, b + 2 : b + 2 + R], sems.at[2 + b // R]))
        stores[-1].start()
    for store in stores:
        store.wait()


def middle(stats, vecs, img, cot, ce, co, k1, k2):
    H, W, C = img.shape[1:]
    return pl.pallas_call(
        middle_kernel,
        out_shape=(jax.ShapeDtypeStruct(img.shape, BF16), jax.ShapeDtypeStruct((3, 4, W, C), BF16)),
        in_specs=[(SMEM,) * 4, (VMEM,) * 5] + [VMEM] * 4 + [HBM, HBM],
        out_specs=(HBM, VMEM),
        scratch_shapes=[
            pltpu.VMEM((4, PADW + 16, C), F32),
            pltpu.VMEM((3, H, PADW, C), BF16),
            pltpu.VMEM((3, H, PADW, C), BF16),
            pltpu.VMEM((3, H - 2, W, C), BF16),
            pltpu.VMEM((H - 4, W, C), BF16),
            pltpu.VMEM((2, 2 * H, C), F32),
            pltpu.VMEM((2, 2 * H, C), F32),
            pltpu.VMEM(k1.shape, BF16),
            pltpu.VMEM(k2.shape, BF16),
            pltpu.SemaphoreType.DMA((4,)),
        ],
        compiler_params=LIMIT,
        name="middle",
    )(stats, vecs, img, cot, ce, co, k1, k2)


def border_kernel(
    stats, vecs, img, cot, ce, co, odd, even, w1, w2, kept, old, out,
    rowbuf, act3, cot3, in3, res, nbuf, fbuf, k1, k2, sems,
):
    H, W, C = img.shape[1:]
    m = 2 * H
    loads = [pltpu.make_async_copy(w1, k1, sems.at[0]), pltpu.make_async_copy(w2, k2, sems.at[1])]
    for load in loads:
        load.start()
    half_one, bias_one, half_two, bias_two = affine(stats, vecs, C)
    odd_row, odd_col, (up, down, to_left, to_right) = place()
    for k in range(2):
        nbuf[k, 4 : m + 4], fbuf[k, 4 : m + 4] = ce[k].astype(F32), co[k].astype(F32)
        o, e = odd[k, 2 * W : 2 * W + 16].astype(F32), even[k, 2 * W : 2 * W + 16].astype(F32)
        near_odd, near_even, far_odd, far_even = o[0:4], e[0:4], o[4:8], e[4:8]
        nbuf[k, 0:4] = jnp.where(odd_row, near_even, near_odd)
        nbuf[k, m + 4 : m + 8] = jnp.where(odd_row, near_odd, near_even)
        fbuf[k, 0:4] = jnp.where(odd_row, far_even, far_odd)
        fbuf[k, m + 4 : m + 8] = jnp.where(odd_row, far_odd, far_even)
    count = 0
    for s, h in enumerate((0, 1, 2, 3, H, H + 1, H + 2, H + 3)):
        for k, (src, dst) in enumerate(((img, act3), (cot, cot3))):
            mask = None
            if h < 2 or h >= H + 2:
                t = h if h < 2 else h - H - 2
                cut = slice(t * W, (t + 1) * W)
                o, e = odd[k, cut], even[k, cut]
                own = jnp.where(odd_row, e, o) if h < 2 else jnp.where(odd_row, o, e)
                mask = up if h < 2 else down
            else:
                own = src[0, h - 2]
            near, far = nbuf[k, 2 * h : 2 * h + 2], fbuf[k, 2 * h : 2 * h + 2]
            lft, rgt = jnp.where(odd_col, near, far), jnp.where(odd_col, far, near)
            if k == 0:
                own = act_of(own, half_one, bias_one)
                lft, rgt = act_of(lft, half_one, bias_one) * to_left, act_of(rgt, half_one, bias_one) * to_right
                if mask is not None:
                    own, lft, rgt = own * mask, lft * mask, rgt * mask
            fill(rowbuf.at[count % 4], own, lft, rgt, dst, s)
            count += 1
    for j in range(3):
        for s, d in enumerate((2, 3, 4, 5)):
            in3[j, d] = kept[j, s]
    for load in loads:
        load.wait()
    cmask = col_mask(to_left, to_right, W)
    c1 = conv(act3, k1, (0, 4), 2, PADW, False)
    c2 = conv(cot3, k2, (0, 4), 2, PADW, True)
    for r, (d, mask) in enumerate(((0, up), (1, None), (6, None), (7, down))):
        g = inner_rows(c1, c2, r, half_two, bias_two, cmask)
        store_inner(rowbuf.at[r], g if mask is None else g * mask, in3, d, W)
    c3 = conv(in3, k1, (0, 4), 2, W, True)
    for r, h in enumerate((0, 1, H - 2, H - 1)):
        res[r] = result_row(img[0, h], cot[0, h], c3[r * W : (r + 1) * W], half_one, bias_one)
    stores = [
        pltpu.make_async_copy(res.at[0:2], out.at[0, 0:2], sems.at[2]),
        pltpu.make_async_copy(res.at[2:4], out.at[0, H - 2 : H], sems.at[3]),
    ]
    for store in stores:
        store.start()
    for store in stores:
        store.wait()


def border(stats, vecs, img, cot, ce, co, odd, even, k1, k2, kept, old):
    H, W, C = img.shape[1:]
    return pl.pallas_call(
        border_kernel,
        out_shape=jax.ShapeDtypeStruct(img.shape, BF16),
        in_specs=[(SMEM,) * 4, (VMEM,) * 5] + [VMEM] * 6 + [HBM, HBM, VMEM, HBM],
        out_specs=HBM,
        input_output_aliases={4 + 5 + 6 + 3: 0},
        scratch_shapes=[
            pltpu.VMEM((4, PADW + 16, C), F32),
            pltpu.VMEM((3, 8, PADW, C), BF16),
            pltpu.VMEM((3, 8, PADW, C), BF16),
            pltpu.VMEM((3, 8, W, C), BF16),
            pltpu.VMEM((4, W, C), BF16),
            pltpu.VMEM((2, 2 * H + 8, C), F32),
            pltpu.VMEM((2, 2 * H + 8, C), F32),
            pltpu.VMEM(k1.shape, BF16),
            pltpu.VMEM(k2.shape, BF16),
            pltpu.SemaphoreType.DMA((4,)),
        ],
        compiler_params=LIMIT,
        name="border",
    )(stats, vecs, img, cot, ce, co, odd, even, k1, k2, kept, old)


def swaps(size, first):
    return [pair for i in range(first, size - 1, 2) for pair in ((i, i + 1), (i + 1, i))]


def per_device(
    image_in,
    cotangent,
    first_kernel,
    first_bias,
    second_kernel,
    first_center,
    first_inverse,
    first_gain,
    first_shift,
    second_center,
    second_inverse,
    second_gain,
    second_shift,
):
    stats = (first_center, first_inverse, second_center, second_inverse)
    vecs = tuple(v[None] for v in (first_bias, first_gain, first_shift, second_gain, second_shift))
    def send(name, x):
        axis = COLS if name[0] == "c" else ROWS
        return lax.ppermute(x, axis, swaps(lax.axis_size(axis), int(name[1] == "o")))

    stay = lambda x: pltpu.with_memory_space_constraint(x, pltpu.HBM)
    first_kernel, second_kernel = stay(first_kernel), stay(second_kernel)
    near, far = edges(image_in, cotangent)
    co, ce = send("co", far), send("ce", near)
    odd, even, ce, co = messages(image_in, cotangent, ce, co)
    odd, even = send("ro", odd), send("re", even)
    out, kept = middle(stats, vecs, image_in, cotangent, ce, co, first_kernel, second_kernel)
    return border(stats, vecs, image_in, cotangent, ce, co, odd, even, first_kernel, second_kernel, kept, out)


def solution(mesh):
    tiled, whole = P(None, ROWS, COLS, None), P()
    return jax.shard_map(
        per_device,
        mesh=mesh,
        in_specs=(tiled, tiled) + (whole,) * 11,
        out_specs=tiled,
        check_vma=False,
    )
```

```python
import jax
import jax.numpy as jnp
from jax import lax
from jax.experimental import pallas as pl
from jax.experimental.pallas import tpu as pltpu
from jax.sharding import PartitionSpec as P

PADW = 112
F32, BF16 = jnp.float32, jnp.bfloat16
ROWS, COLS = "rows", "cols"
VMEM, HBM, SMEM = (pl.BlockSpec(memory_space=m) for m in (pltpu.VMEM, pltpu.HBM, pltpu.SMEM))
SMALL, LARGE = (pltpu.CompilerParams(vmem_limit_bytes=n << 20) for n in (4, 20))


def place():
    row, col = lax.axis_index(ROWS), lax.axis_index(COLS)
    rows, cols = lax.axis_size(ROWS), lax.axis_size(COLS)
    exists = [x.astype(jnp.int32).astype(F32) for x in (row > 0, row < rows - 1, col > 0, col < cols - 1)]
    return row % 2 == 1, col % 2 == 1, exists


def edges_kernel(img, cot, near, far, lo, hi, strip, sems):
    H, W, _ = img.shape[1:]
    copies = []
    for k, x in enumerate((img, cot)):
        copies += [
            pltpu.make_async_copy(x.at[0, :, 0:8, :], lo.at[k], sems.at[2 * k]),
            pltpu.make_async_copy(x.at[0, :, W - 8 : W, :], hi.at[k], sems.at[2 * k + 1]),
        ]
    for c in copies:
        c.start()
    _, odd_col, _ = place()
    for k in range(2):
        copies[2 * k].wait()
        copies[2 * k + 1].wait()
        for h in range(H):
            strip[0, 2 * h : 2 * h + 2, :] = lo[k, h].astype(F32)[0:2]
            strip[1, 2 * h : 2 * h + 2, :] = hi[k, h].astype(F32)[6:8]
        first, last = strip[0].astype(BF16), strip[1].astype(BF16)
        near[k] = jnp.where(odd_col, first, last)
        far[k] = jnp.where(odd_col, last, first)


def edges(img, cot):
    H, _, C = img.shape[1:]
    shape = jax.ShapeDtypeStruct((2, 2 * H, C), BF16)
    return pl.pallas_call(
        edges_kernel,
        out_shape=(shape, shape),
        in_specs=[HBM, HBM],
        out_specs=(VMEM, VMEM),
        scratch_shapes=[
            pltpu.VMEM((2, H, 8, C), BF16),
            pltpu.VMEM((2, H, 8, C), BF16),
            pltpu.VMEM((2, 2 * H, C), F32),
            pltpu.SemaphoreType.DMA((4,)),
        ],
        compiler_params=SMALL,
        name="edges",
    )(img, cot)


def messages_kernel(img, cot, ce, co, odd, even, buf):
    H, W = img.shape[1], img.shape[2]
    n, m = 2 * W, ce.shape[1]
    odd_row, _, _ = place()
    buf[8:16] = jnp.zeros_like(buf[8:16])
    for k in range(2):
        x = (img, cot)[k]
        for h in range(2):
            upper, lower = x[0, h], x[0, H - 2 + h]
            odd[k, h * W : (h + 1) * W] = jnp.where(odd_row, lower, upper)
            even[k, h * W : (h + 1) * W] = jnp.where(odd_row, upper, lower)
        tops = [r[k, 0:16].astype(F32)[0:4] for r in (ce, co)]
        ends = [r[k, m - 16 : m].astype(F32)[12:16] for r in (ce, co)]
        for dst, flip in ((odd, False), (even, True)):
            for s in range(2):
                first, second = (tops[s], ends[s]) if flip else (ends[s], tops[s])
                buf[4 * s : 4 * s + 4] = jnp.where(odd_row, first, second)
            dst[k, n : n + 16] = buf[...].astype(BF16)


def messages(img, cot, ce, co):
    n, C = 2 * img.shape[2], ce.shape[2]
    shape = lambda n: jax.ShapeDtypeStruct((2, n, C), BF16)
    return pl.pallas_call(
        messages_kernel,
        out_shape=(shape(n + 16), shape(n + 16)),
        in_specs=[VMEM] * 4,
        out_specs=(VMEM,) * 2,
        scratch_shapes=[pltpu.VMEM((16, C), F32)],
        compiler_params=SMALL,
        name="messages",
    )(img, cot, ce, co)


def per_channel(stat, channels):
    group = lax.broadcasted_iota(jnp.int32, (1, channels), 1) // (channels // stat.shape[0])
    wide = jnp.full((1, channels), stat[0], F32)
    for g in range(1, stat.shape[0]):
        wide = jnp.where(group == g, stat[g], wide)
    return wide


def affine(stats, vecs, C):
    center_one, inverse_one, center_two, inverse_two = (per_channel(v, C) for v in stats)
    bias, gain_one, shift_one, gain_two, shift_two = (v[0:1, :] for v in vecs)
    half_one, half_two = 0.5 * (inverse_one * gain_one), 0.5 * (inverse_two * gain_two)
    bias_one = 0.5 * shift_one - center_one * half_one
    bias_two = (bias - center_two) * half_two + 0.5 * shift_two
    return half_one, bias_one, half_two, bias_two


def act_of(x, half, bias):
    h = x.astype(F32) * half + bias
    return h * jnp.tanh(h) + h


def slope_of(v):
    t = jnp.tanh(v)
    return (1.0 + t) * (1.0 + v - v * t)


def fill(rb, own, lft, rgt, dst, h):
    W = own.shape[0]
    rb[2 : 2 + W, :] = own.astype(F32)
    rb[0:2, :] = lft
    rb[2 + W : 4 + W, :] = rgt
    for j in range(3):
        dst[j, h, :, :] = rb[j : j + PADW, :].astype(BF16)


def conv(src, wref, starts, rows, width, flip):
    C, acc = wref.shape[3], None
    for i in range(3):
        for j in range(3):
            parts = [src[j, b + i : b + i + rows, 0:width, :].reshape(rows * width, C) for b in starts]
            lhs = parts[0] if len(parts) == 1 else jnp.concatenate(parts)
            w = wref[2 - i, 2 - j] if flip else wref[i, j]
            dims = (((1,), (1 if flip else 0,)), ((), ()))
            t = lax.dot_general(lhs, w, dims, preferred_element_type=F32)
            acc = t if acc is None else acc + t
    return acc


def inner_rows(c1, c2, r, half_two, bias_two, cmask):
    cut = slice(r * PADW, (r + 1) * PADW)
    return c2[cut] * half_two * slope_of(c1[cut] * half_two + bias_two) * cmask


def store_inner(rb, g, dst, h, W):
    rb[0:PADW, :] = g
    for j in range(3):
        dst[j, h, :, :] = rb[j : j + W, :].astype(BF16)


def col_mask(to_left, to_right, W):
    pos = lax.broadcasted_iota(jnp.int32, (PADW, 1), 0)
    return jnp.where(pos == 0, to_left, jnp.where(pos == W + 1, to_right, 1.0))


def result_row(x, g, c3, half_one, bias_one):
    v = x.astype(F32) * half_one + bias_one
    return (g.astype(F32) + c3 * half_one * slope_of(v)).astype(BF16)


def middle_kernel(
    stats, vecs, img, cot, ce, co, k1, k2, out, kept, rowbuf, act3, cot3, in3, res, nbuf, fbuf, sems
):
    H, W, C = img.shape[1:]
    half_one, bias_one, half_two, bias_two = affine(stats, vecs, C)
    odd_row, odd_col, (up, down, to_left, to_right) = place()
    for k in range(2):
        nbuf[k], fbuf[k] = ce[k].astype(F32), co[k].astype(F32)
    count = 0
    for h in range(H):
        for k, (src, dst) in enumerate(((img, act3), (cot, cot3))):
            cut = slice(2 * h, 2 * h + 2)
            near, far = nbuf[k, cut], fbuf[k, cut]
            lft, rgt = jnp.where(odd_col, near, far), jnp.where(odd_col, far, near)
            own = src[0, h]
            if k == 0:
                own = act_of(own, half_one, bias_one)
                lft, rgt = act_of(lft, half_one, bias_one) * to_left, act_of(rgt, half_one, bias_one) * to_right
            fill(rowbuf.at[count % 4], own, lft, rgt, dst, h)
            count += 1
    cmask = col_mask(to_left, to_right, W)
    R = (H - 2) // 2
    for b in range(0, H - 2, R):
        c1 = conv(act3, k1, (b,), R, PADW, False)
        c2 = conv(cot3, k2, (b,), R, PADW, True)
        for r in range(R):
            g = inner_rows(c1, c2, r, half_two, bias_two, cmask)
            store_inner(rowbuf.at[r % 4], g, in3, b + r, W)
    for j in range(3):
        for s, h in enumerate((0, 1, H - 4, H - 3)):
            kept[j, s] = in3[j, h]
    R = (H - 4) // 2
    stores = []
    for b in range(0, H - 4, R):
        c3 = conv(in3, k1, (b,), R, W, True)
        for r in range(R):
            h = b + r + 2
            res[b + r] = result_row(img[0, h], cot[0, h], c3[r * W : (r + 1) * W], half_one, bias_one)
        stores.append(pltpu.make_async_copy(res.at[b : b + R], out.at[0, b + 2 : b + 2 + R], sems.at[2 + b // R]))
        stores[-1].start()
    for store in stores:
        store.wait()


def middle(stats, vecs, img, cot, ce, co, k1, k2):
    H, W, C = img.shape[1:]
    return pl.pallas_call(
        middle_kernel,
        out_shape=(jax.ShapeDtypeStruct(img.shape, BF16), jax.ShapeDtypeStruct((3, 4, W, C), BF16)),
        in_specs=[(SMEM,) * 4, (VMEM,) * 5] + [VMEM] * 6,
        out_specs=(HBM, VMEM),
        scratch_shapes=[
            pltpu.VMEM((4, PADW + 16, C), F32),
            pltpu.VMEM((3, H, PADW, C), BF16),
            pltpu.VMEM((3, H, PADW, C), BF16),
            pltpu.VMEM((3, H - 2, W, C), BF16),
            pltpu.VMEM((H - 4, W, C), BF16),
            pltpu.VMEM((2, 2 * H, C), F32),
            pltpu.VMEM((2, 2 * H, C), F32),
            pltpu.SemaphoreType.DMA((4,)),
        ],
        compiler_params=LARGE,
        name="middle",
    )(stats, vecs, img, cot, ce, co, k1, k2)


def border_kernel(
    stats, vecs, img, cot, ce, co, odd, even, k1, k2, kept, old, out,
    rowbuf, act3, cot3, in3, res, nbuf, fbuf, sems,
):
    H, W, C = img.shape[1:]
    m = 2 * H
    half_one, bias_one, half_two, bias_two = affine(stats, vecs, C)
    odd_row, odd_col, (up, down, to_left, to_right) = place()
    for k in range(2):
        nbuf[k, 4 : m + 4], fbuf[k, 4 : m + 4] = ce[k].astype(F32), co[k].astype(F32)
        o, e = odd[k, 2 * W : 2 * W + 16].astype(F32), even[k, 2 * W : 2 * W + 16].astype(F32)
        near_odd, near_even, far_odd, far_even = o[0:4], e[0:4], o[4:8], e[4:8]
        nbuf[k, 0:4] = jnp.where(odd_row, near_even, near_odd)
        nbuf[k, m + 4 : m + 8] = jnp.where(odd_row, near_odd, near_even)
        fbuf[k, 0:4] = jnp.where(odd_row, far_even, far_odd)
        fbuf[k, m + 4 : m + 8] = jnp.where(odd_row, far_odd, far_even)
    count = 0
    for s, h in enumerate((0, 1, 2, 3, H, H + 1, H + 2, H + 3)):
        for k, (src, dst) in enumerate(((img, act3), (cot, cot3))):
            mask = None
            if h < 2 or h >= H + 2:
                t = h if h < 2 else h - H - 2
                cut = slice(t * W, (t + 1) * W)
                o, e = odd[k, cut], even[k, cut]
                own = jnp.where(odd_row, e, o) if h < 2 else jnp.where(odd_row, o, e)
                mask = up if h < 2 else down
            else:
                own = src[0, h - 2]
            near, far = nbuf[k, 2 * h : 2 * h + 2], fbuf[k, 2 * h : 2 * h + 2]
            lft, rgt = jnp.where(odd_col, near, far), jnp.where(odd_col, far, near)
            if k == 0:
                own = act_of(own, half_one, bias_one)
                lft, rgt = act_of(lft, half_one, bias_one) * to_left, act_of(rgt, half_one, bias_one) * to_right
                if mask is not None:
                    own, lft, rgt = own * mask, lft * mask, rgt * mask
            fill(rowbuf.at[count % 4], own, lft, rgt, dst, s)
            count += 1
    for j in range(3):
        for s, d in enumerate((2, 3, 4, 5)):
            in3[j, d] = kept[j, s]
    cmask = col_mask(to_left, to_right, W)
    c1 = conv(act3, k1, (0, 4), 2, PADW, False)
    c2 = conv(cot3, k2, (0, 4), 2, PADW, True)
    for r, (d, mask) in enumerate(((0, up), (1, None), (6, None), (7, down))):
        g = inner_rows(c1, c2, r, half_two, bias_two, cmask)
        store_inner(rowbuf.at[r], g if mask is None else g * mask, in3, d, W)
    c3 = conv(in3, k1, (0, 4), 2, W, True)
    for r, h in enumerate((0, 1, H - 2, H - 1)):
        res[r] = result_row(img[0, h], cot[0, h], c3[r * W : (r + 1) * W], half_one, bias_one)
    stores = [
        pltpu.make_async_copy(res.at[0:2], out.at[0, 0:2], sems.at[2]),
        pltpu.make_async_copy(res.at[2:4], out.at[0, H - 2 : H], sems.at[3]),
    ]
    for store in stores:
        store.start()
    for store in stores:
        store.wait()


def border(stats, vecs, img, cot, ce, co, odd, even, k1, k2, kept, old):
    H, W, C = img.shape[1:]
    return pl.pallas_call(
        border_kernel,
        out_shape=jax.ShapeDtypeStruct(img.shape, BF16),
        in_specs=[(SMEM,) * 4, (VMEM,) * 5] + [VMEM] * 9 + [HBM],
        out_specs=HBM,
        input_output_aliases={4 + 5 + 6 + 3: 0},
        scratch_shapes=[
            pltpu.VMEM((4, PADW + 16, C), F32),
            pltpu.VMEM((3, 8, PADW, C), BF16),
            pltpu.VMEM((3, 8, PADW, C), BF16),
            pltpu.VMEM((3, 8, W, C), BF16),
            pltpu.VMEM((4, W, C), BF16),
            pltpu.VMEM((2, 2 * H + 8, C), F32),
            pltpu.VMEM((2, 2 * H + 8, C), F32),
            pltpu.SemaphoreType.DMA((4,)),
        ],
        compiler_params=LARGE,
        name="border",
    )(stats, vecs, img, cot, ce, co, odd, even, k1, k2, kept, old)


def swaps(size, first):
    return [pair for i in range(first, size - 1, 2) for pair in ((i, i + 1), (i + 1, i))]


def per_device(
    image_in,
    cotangent,
    first_kernel,
    first_bias,
    second_kernel,
    first_center,
    first_inverse,
    first_gain,
    first_shift,
    second_center,
    second_inverse,
    second_gain,
    second_shift,
):
    stats = (first_center, first_inverse, second_center, second_inverse)
    vecs = tuple(v[None] for v in (first_bias, first_gain, first_shift, second_gain, second_shift))
    def send(name, x):
        axis = COLS if name[0] == "c" else ROWS
        return lax.ppermute(x, axis, swaps(lax.axis_size(axis), int(name[1] == "o")))

    near, far = edges(image_in, cotangent)
    co, ce = send("co", far), send("ce", near)
    odd, even = messages(image_in, cotangent, ce, co)
    odd, even = send("ro", odd), send("re", even)
    out, kept = middle(stats, vecs, image_in, cotangent, ce, co, first_kernel, second_kernel)
    return border(stats, vecs, image_in, cotangent, ce, co, odd, even, first_kernel, second_kernel, kept, out)


def solution(mesh):
    tiled, whole = P(None, ROWS, COLS, None), P()
    return jax.shard_map(
        per_device,
        mesh=mesh,
        in_specs=(tiled, tiled) + (whole,) * 11,
        out_specs=tiled,
        check_vma=False,
    )
```

```python
import jax
import jax.numpy as jnp
from jax import lax
from jax.experimental import pallas as pl
from jax.experimental.pallas import tpu as pltpu
from jax.sharding import PartitionSpec as P

PADW = 112
F32, BF16 = jnp.float32, jnp.bfloat16
ROWS, COLS = "rows", "cols"
VMEM, HBM, SMEM = (pl.BlockSpec(memory_space=m) for m in (pltpu.VMEM, pltpu.HBM, pltpu.SMEM))
SMALL, LARGE = (pltpu.CompilerParams(vmem_limit_bytes=n << 20) for n in (4, 20))


def place():
    row, col = lax.axis_index(ROWS), lax.axis_index(COLS)
    rows, cols = lax.axis_size(ROWS), lax.axis_size(COLS)
    exists = [x.astype(jnp.int32).astype(F32) for x in (row > 0, row < rows - 1, col > 0, col < cols - 1)]
    return row % 2 == 1, col % 2 == 1, exists


def edges_kernel(img, cot, near, far, lo, hi, strip, sems):
    H, W, _ = img.shape[1:]
    copies = []
    for k, x in enumerate((img, cot)):
        copies += [
            pltpu.make_async_copy(x.at[0, :, 0:8, :], lo.at[k], sems.at[2 * k]),
            pltpu.make_async_copy(x.at[0, :, W - 8 : W, :], hi.at[k], sems.at[2 * k + 1]),
        ]
    for c in copies:
        c.start()
    _, odd_col, _ = place()
    for k in range(2):
        copies[2 * k].wait()
        copies[2 * k + 1].wait()
        for h in range(H):
            strip[0, 2 * h : 2 * h + 2, :] = lo[k, h].astype(F32)[0:2]
            strip[1, 2 * h : 2 * h + 2, :] = hi[k, h].astype(F32)[6:8]
        first, last = strip[0].astype(BF16), strip[1].astype(BF16)
        near[k] = jnp.where(odd_col, first, last)
        far[k] = jnp.where(odd_col, last, first)


def edges(img, cot):
    H, _, C = img.shape[1:]
    shape = jax.ShapeDtypeStruct((2, 2 * H, C), BF16)
    return pl.pallas_call(
        edges_kernel,
        out_shape=(shape, shape),
        in_specs=[HBM, HBM],
        out_specs=(VMEM, VMEM),
        scratch_shapes=[
            pltpu.VMEM((2, H, 8, C), BF16),
            pltpu.VMEM((2, H, 8, C), BF16),
            pltpu.VMEM((2, 2 * H, C), F32),
            pltpu.SemaphoreType.DMA((4,)),
        ],
        compiler_params=SMALL,
        name="edges",
    )(img, cot)


def messages_kernel(img, cot, ce, co, odd, even, buf):
    H, W = img.shape[1], img.shape[2]
    n, m = 2 * W, ce.shape[1]
    odd_row, _, _ = place()
    buf[8:16] = jnp.zeros_like(buf[8:16])
    for k in range(2):
        x = (img, cot)[k]
        for h in range(2):
            upper, lower = x[0, h], x[0, H - 2 + h]
            odd[k, h * W : (h + 1) * W] = jnp.where(odd_row, lower, upper)
            even[k, h * W : (h + 1) * W] = jnp.where(odd_row, upper, lower)
        tops = [r[k, 0:16].astype(F32)[0:4] for r in (ce, co)]
        ends = [r[k, m - 16 : m].astype(F32)[12:16] for r in (ce, co)]
        for dst, flip in ((odd, False), (even, True)):
            for s in range(2):
                first, second = (tops[s], ends[s]) if flip else (ends[s], tops[s])
                buf[4 * s : 4 * s + 4] = jnp.where(odd_row, first, second)
            dst[k, n : n + 16] = buf[...].astype(BF16)


def messages(img, cot, ce, co):
    n, C = 2 * img.shape[2], ce.shape[2]
    shape = lambda n: jax.ShapeDtypeStruct((2, n, C), BF16)
    return pl.pallas_call(
        messages_kernel,
        out_shape=(shape(n + 16), shape(n + 16)),
        in_specs=[VMEM] * 4,
        out_specs=(VMEM,) * 2,
        scratch_shapes=[pltpu.VMEM((16, C), F32)],
        compiler_params=SMALL,
        name="messages",
    )(img, cot, ce, co)


def per_channel(stat, channels):
    group = lax.broadcasted_iota(jnp.int32, (1, channels), 1) // (channels // stat.shape[0])
    wide = jnp.full((1, channels), stat[0], F32)
    for g in range(1, stat.shape[0]):
        wide = jnp.where(group == g, stat[g], wide)
    return wide


def affine(stats, vecs, C):
    center_one, inverse_one, center_two, inverse_two = (per_channel(v, C) for v in stats)
    bias, gain_one, shift_one, gain_two, shift_two = (v[0:1, :] for v in vecs)
    half_one, half_two = 0.5 * (inverse_one * gain_one), 0.5 * (inverse_two * gain_two)
    bias_one = 0.5 * shift_one - center_one * half_one
    bias_two = (bias - center_two) * half_two + 0.5 * shift_two
    return half_one, bias_one, half_two, bias_two


def act_of(x, half, bias):
    h = x.astype(F32) * half + bias
    return h * jnp.tanh(h) + h


def slope_of(v):
    t = jnp.tanh(v)
    return (1.0 + t) * (1.0 + v - v * t)


def fill(rb, own, lft, rgt, dst, h):
    W = own.shape[0]
    rb[2 : 2 + W, :] = own.astype(F32)
    rb[0:2, :] = lft
    rb[2 + W : 4 + W, :] = rgt
    for j in range(3):
        dst[j, h, :, :] = rb[j : j + PADW, :].astype(BF16)


def conv(src, wref, starts, rows, width, flip):
    C, acc = wref.shape[3], None
    for i in range(3):
        for j in range(3):
            parts = [src[j, b + i : b + i + rows, 0:width, :].reshape(rows * width, C) for b in starts]
            lhs = parts[0] if len(parts) == 1 else jnp.concatenate(parts)
            w = wref[2 - i, 2 - j] if flip else wref[i, j]
            dims = (((1,), (1 if flip else 0,)), ((), ()))
            t = lax.dot_general(lhs, w, dims, preferred_element_type=F32)
            acc = t if acc is None else acc + t
    return acc


def inner_rows(c1, c2, r, half_two, bias_two, cmask):
    cut = slice(r * PADW, (r + 1) * PADW)
    return c2[cut] * half_two * slope_of(c1[cut] * half_two + bias_two) * cmask


def store_inner(rb, g, dst, h, W):
    rb[0:PADW, :] = g
    for j in range(3):
        dst[j, h, :, :] = rb[j : j + W, :].astype(BF16)


def col_mask(to_left, to_right, W):
    pos = lax.broadcasted_iota(jnp.int32, (PADW, 1), 0)
    return jnp.where(pos == 0, to_left, jnp.where(pos == W + 1, to_right, 1.0))


def result_row(x, g, c3, half_one, bias_one):
    v = x.astype(F32) * half_one + bias_one
    return (g.astype(F32) + c3 * half_one * slope_of(v)).astype(BF16)


def middle_kernel(
    stats, vecs, img, cot, ce, co, k1, w2, out, kept, rowbuf, act3, cot3, in3, res, nbuf, fbuf, k2, sems
):
    H, W, C = img.shape[1:]
    load = pltpu.make_async_copy(w2, k2, sems.at[0])
    load.start()
    half_one, bias_one, half_two, bias_two = affine(stats, vecs, C)
    odd_row, odd_col, (up, down, to_left, to_right) = place()
    for k in range(2):
        nbuf[k], fbuf[k] = ce[k].astype(F32), co[k].astype(F32)
    count = 0
    for h in range(H):
        for k, (src, dst) in enumerate(((img, act3), (cot, cot3))):
            cut = slice(2 * h, 2 * h + 2)
            near, far = nbuf[k, cut], fbuf[k, cut]
            lft, rgt = jnp.where(odd_col, near, far), jnp.where(odd_col, far, near)
            own = src[0, h]
            if k == 0:
                own = act_of(own, half_one, bias_one)
                lft, rgt = act_of(lft, half_one, bias_one) * to_left, act_of(rgt, half_one, bias_one) * to_right
            fill(rowbuf.at[count % 4], own, lft, rgt, dst, h)
            count += 1
    load.wait()
    cmask = col_mask(to_left, to_right, W)
    R = (H - 2) // 2
    for b in range(0, H - 2, R):
        c1 = conv(act3, k1, (b,), R, PADW, False)
        c2 = conv(cot3, k2, (b,), R, PADW, True)
        for r in range(R):
            g = inner_rows(c1, c2, r, half_two, bias_two, cmask)
            store_inner(rowbuf.at[r % 4], g, in3, b + r, W)
    for j in range(3):
        for s, h in enumerate((0, 1, H - 4, H - 3)):
            kept[j, s] = in3[j, h]
    R = (H - 4) // 2
    stores = []
    for b in range(0, H - 4, R):
        c3 = conv(in3, k1, (b,), R, W, True)
        for r in range(R):
            h = b + r + 2
            res[b + r] = result_row(img[0, h], cot[0, h], c3[r * W : (r + 1) * W], half_one, bias_one)
        stores.append(pltpu.make_async_copy(res.at[b : b + R], out.at[0, b + 2 : b + 2 + R], sems.at[2 + b // R]))
        stores[-1].start()
    for store in stores:
        store.wait()


def middle(stats, vecs, img, cot, ce, co, k1, k2):
    H, W, C = img.shape[1:]
    return pl.pallas_call(
        middle_kernel,
        out_shape=(jax.ShapeDtypeStruct(img.shape, BF16), jax.ShapeDtypeStruct((3, 4, W, C), BF16)),
        in_specs=[(SMEM,) * 4, (VMEM,) * 5] + [VMEM] * 5 + [HBM],
        out_specs=(HBM, VMEM),
        scratch_shapes=[
            pltpu.VMEM((4, PADW + 16, C), F32),
            pltpu.VMEM((3, H, PADW, C), BF16),
            pltpu.VMEM((3, H, PADW, C), BF16),
            pltpu.VMEM((3, H - 2, W, C), BF16),
            pltpu.VMEM((H - 4, W, C), BF16),
            pltpu.VMEM((2, 2 * H, C), F32),
            pltpu.VMEM((2, 2 * H, C), F32),
            pltpu.VMEM(k2.shape, BF16),
            pltpu.SemaphoreType.DMA((4,)),
        ],
        compiler_params=LARGE,
        name="middle",
    )(stats, vecs, img, cot, ce, co, k1, k2)


def border_kernel(
    stats, vecs, img, cot, ce, co, odd, even, k1, w2, kept, old, out,
    rowbuf, act3, cot3, in3, res, nbuf, fbuf, k2, sems,
):
    H, W, C = img.shape[1:]
    m = 2 * H
    load = pltpu.make_async_copy(w2, k2, sems.at[0])
    load.start()
    half_one, bias_one, half_two, bias_two = affine(stats, vecs, C)
    odd_row, odd_col, (up, down, to_left, to_right) = place()
    for k in range(2):
        nbuf[k, 4 : m + 4], fbuf[k, 4 : m + 4] = ce[k].astype(F32), co[k].astype(F32)
        o, e = odd[k, 2 * W : 2 * W + 16].astype(F32), even[k, 2 * W : 2 * W + 16].astype(F32)
        near_odd, near_even, far_odd, far_even = o[0:4], e[0:4], o[4:8], e[4:8]
        nbuf[k, 0:4] = jnp.where(odd_row, near_even, near_odd)
        nbuf[k, m + 4 : m + 8] = jnp.where(odd_row, near_odd, near_even)
        fbuf[k, 0:4] = jnp.where(odd_row, far_even, far_odd)
        fbuf[k, m + 4 : m + 8] = jnp.where(odd_row, far_odd, far_even)
    count = 0
    for s, h in enumerate((0, 1, 2, 3, H, H + 1, H + 2, H + 3)):
        for k, (src, dst) in enumerate(((img, act3), (cot, cot3))):
            mask = None
            if h < 2 or h >= H + 2:
                t = h if h < 2 else h - H - 2
                cut = slice(t * W, (t + 1) * W)
                o, e = odd[k, cut], even[k, cut]
                own = jnp.where(odd_row, e, o) if h < 2 else jnp.where(odd_row, o, e)
                mask = up if h < 2 else down
            else:
                own = src[0, h - 2]
            near, far = nbuf[k, 2 * h : 2 * h + 2], fbuf[k, 2 * h : 2 * h + 2]
            lft, rgt = jnp.where(odd_col, near, far), jnp.where(odd_col, far, near)
            if k == 0:
                own = act_of(own, half_one, bias_one)
                lft, rgt = act_of(lft, half_one, bias_one) * to_left, act_of(rgt, half_one, bias_one) * to_right
                if mask is not None:
                    own, lft, rgt = own * mask, lft * mask, rgt * mask
            fill(rowbuf.at[count % 4], own, lft, rgt, dst, s)
            count += 1
    for j in range(3):
        for s, d in enumerate((2, 3, 4, 5)):
            in3[j, d] = kept[j, s]
    load.wait()
    cmask = col_mask(to_left, to_right, W)
    c1 = conv(act3, k1, (0, 4), 2, PADW, False)
    c2 = conv(cot3, k2, (0, 4), 2, PADW, True)
    for r, (d, mask) in enumerate(((0, up), (1, None), (6, None), (7, down))):
        g = inner_rows(c1, c2, r, half_two, bias_two, cmask)
        store_inner(rowbuf.at[r], g if mask is None else g * mask, in3, d, W)
    c3 = conv(in3, k1, (0, 4), 2, W, True)
    for r, h in enumerate((0, 1, H - 2, H - 1)):
        res[r] = result_row(img[0, h], cot[0, h], c3[r * W : (r + 1) * W], half_one, bias_one)
    stores = [
        pltpu.make_async_copy(res.at[0:2], out.at[0, 0:2], sems.at[2]),
        pltpu.make_async_copy(res.at[2:4], out.at[0, H - 2 : H], sems.at[3]),
    ]
    for store in stores:
        store.start()
    for store in stores:
        store.wait()


def border(stats, vecs, img, cot, ce, co, odd, even, k1, k2, kept, old):
    H, W, C = img.shape[1:]
    return pl.pallas_call(
        border_kernel,
        out_shape=jax.ShapeDtypeStruct(img.shape, BF16),
        in_specs=[(SMEM,) * 4, (VMEM,) * 5] + [VMEM] * 7 + [HBM, VMEM, HBM],
        out_specs=HBM,
        input_output_aliases={4 + 5 + 6 + 3: 0},
        scratch_shapes=[
            pltpu.VMEM((4, PADW + 16, C), F32),
            pltpu.VMEM((3, 8, PADW, C), BF16),
            pltpu.VMEM((3, 8, PADW, C), BF16),
            pltpu.VMEM((3, 8, W, C), BF16),
            pltpu.VMEM((4, W, C), BF16),
            pltpu.VMEM((2, 2 * H + 8, C), F32),
            pltpu.VMEM((2, 2 * H + 8, C), F32),
            pltpu.VMEM(k2.shape, BF16),
            pltpu.SemaphoreType.DMA((4,)),
        ],
        compiler_params=LARGE,
        name="border",
    )(stats, vecs, img, cot, ce, co, odd, even, k1, k2, kept, old)


def swaps(size, first):
    return [pair for i in range(first, size - 1, 2) for pair in ((i, i + 1), (i + 1, i))]


def per_device(
    image_in,
    cotangent,
    first_kernel,
    first_bias,
    second_kernel,
    first_center,
    first_inverse,
    first_gain,
    first_shift,
    second_center,
    second_inverse,
    second_gain,
    second_shift,
):
    stats = (first_center, first_inverse, second_center, second_inverse)
    vecs = tuple(v[None] for v in (first_bias, first_gain, first_shift, second_gain, second_shift))
    def send(name, x):
        axis = COLS if name[0] == "c" else ROWS
        return lax.ppermute(x, axis, swaps(lax.axis_size(axis), int(name[1] == "o")))

    stay = lambda x: pltpu.with_memory_space_constraint(x, pltpu.HBM)
    second_kernel = stay(second_kernel)
    near, far = edges(stay(image_in), stay(cotangent))
    co, ce = send("co", far), send("ce", near)
    odd, even = messages(image_in, cotangent, ce, co)
    odd, even = send("ro", odd), send("re", even)
    out, kept = middle(stats, vecs, image_in, cotangent, ce, co, first_kernel, second_kernel)
    return border(stats, vecs, image_in, cotangent, ce, co, odd, even, first_kernel, second_kernel, kept, out)


def solution(mesh):
    tiled, whole = P(None, ROWS, COLS, None), P()
    return jax.shard_map(
        per_device,
        mesh=mesh,
        in_specs=(tiled, tiled) + (whole,) * 11,
        out_specs=tiled,
        check_vma=False,
    )
```

```python
import jax
import jax.numpy as jnp
from jax import lax
from jax.experimental import pallas as pl
from jax.experimental.pallas import tpu as pltpu
from jax.sharding import PartitionSpec as P

PADW = 112
F32, BF16 = jnp.float32, jnp.bfloat16
ROWS, COLS = "rows", "cols"
VMEM, HBM, SMEM = (pl.BlockSpec(memory_space=m) for m in (pltpu.VMEM, pltpu.HBM, pltpu.SMEM))
SMALL, LARGE = (pltpu.CompilerParams(vmem_limit_bytes=n << 20) for n in (4, 20))


def place():
    row, col = lax.axis_index(ROWS), lax.axis_index(COLS)
    rows, cols = lax.axis_size(ROWS), lax.axis_size(COLS)
    exists = [x.astype(jnp.int32).astype(F32) for x in (row > 0, row < rows - 1, col > 0, col < cols - 1)]
    return row % 2 == 1, col % 2 == 1, exists


def edges_kernel(img, cot, near, far, lo, hi, strip, sems):
    H, W, _ = img.shape[1:]
    copies = []
    for k, x in enumerate((img, cot)):
        copies += [
            pltpu.make_async_copy(x.at[0, :, 0:8, :], lo.at[k], sems.at[2 * k]),
            pltpu.make_async_copy(x.at[0, :, W - 8 : W, :], hi.at[k], sems.at[2 * k + 1]),
        ]
    for c in copies:
        c.start()
    _, odd_col, _ = place()
    for k in range(2):
        copies[2 * k].wait()
        copies[2 * k + 1].wait()
        for h in range(H):
            strip[0, 2 * h : 2 * h + 2, :] = lo[k, h].astype(F32)[0:2]
            strip[1, 2 * h : 2 * h + 2, :] = hi[k, h].astype(F32)[6:8]
        first, last = strip[0].astype(BF16), strip[1].astype(BF16)
        near[k] = jnp.where(odd_col, first, last)
        far[k] = jnp.where(odd_col, last, first)


def edges(img, cot):
    H, _, C = img.shape[1:]
    shape = jax.ShapeDtypeStruct((2, 2 * H, C), BF16)
    return pl.pallas_call(
        edges_kernel,
        out_shape=(shape, shape),
        in_specs=[HBM, HBM],
        out_specs=(VMEM, VMEM),
        scratch_shapes=[
            pltpu.VMEM((2, H, 8, C), BF16),
            pltpu.VMEM((2, H, 8, C), BF16),
            pltpu.VMEM((2, 2 * H, C), F32),
            pltpu.SemaphoreType.DMA((4,)),
        ],
        compiler_params=SMALL,
        name="edges",
    )(img, cot)


def messages_kernel(img, cot, ce, co, odd, even, buf):
    H, W = img.shape[1], img.shape[2]
    n, m = 2 * W, ce.shape[1]
    odd_row, _, _ = place()
    buf[8:16] = jnp.zeros_like(buf[8:16])
    for k in range(2):
        x = (img, cot)[k]
        for h in range(2):
            upper, lower = x[0, h], x[0, H - 2 + h]
            odd[k, h * W : (h + 1) * W] = jnp.where(odd_row, lower, upper)
            even[k, h * W : (h + 1) * W] = jnp.where(odd_row, upper, lower)
        tops = [r[k, 0:16].astype(F32)[0:4] for r in (ce, co)]
        ends = [r[k, m - 16 : m].astype(F32)[12:16] for r in (ce, co)]
        for dst, flip in ((odd, False), (even, True)):
            for s in range(2):
                first, second = (tops[s], ends[s]) if flip else (ends[s], tops[s])
                buf[4 * s : 4 * s + 4] = jnp.where(odd_row, first, second)
            dst[k, n : n + 16] = buf[...].astype(BF16)


def messages(img, cot, ce, co):
    n, C = 2 * img.shape[2], ce.shape[2]
    shape = lambda n: jax.ShapeDtypeStruct((2, n, C), BF16)
    return pl.pallas_call(
        messages_kernel,
        out_shape=(shape(n + 16), shape(n + 16)),
        in_specs=[VMEM] * 4,
        out_specs=(VMEM,) * 2,
        scratch_shapes=[pltpu.VMEM((16, C), F32)],
        compiler_params=SMALL,
        name="messages",
    )(img, cot, ce, co)


def per_channel(stat, channels):
    group = lax.broadcasted_iota(jnp.int32, (1, channels), 1) // (channels // stat.shape[0])
    wide = jnp.full((1, channels), stat[0], F32)
    for g in range(1, stat.shape[0]):
        wide = jnp.where(group == g, stat[g], wide)
    return wide


def affine(stats, vecs, C):
    center_one, inverse_one, center_two, inverse_two = (per_channel(v, C) for v in stats)
    bias, gain_one, shift_one, gain_two, shift_two = (v[0:1, :] for v in vecs)
    half_one, half_two = 0.5 * (inverse_one * gain_one), 0.5 * (inverse_two * gain_two)
    bias_one = 0.5 * shift_one - center_one * half_one
    bias_two = (bias - center_two) * half_two + 0.5 * shift_two
    return half_one, bias_one, half_two, bias_two


def act_of(x, half, bias):
    h = x.astype(F32) * half + bias
    return h * jnp.tanh(h) + h


def slope_of(v):
    t = jnp.tanh(v)
    return (1.0 + t) * (1.0 + v - v * t)


def fill(rb, own, lft, rgt, dst, h):
    W = own.shape[0]
    rb[2 : 2 + W, :] = own.astype(F32)
    rb[0:2, :] = lft
    rb[2 + W : 4 + W, :] = rgt
    for j in range(3):
        dst[j, h, :, :] = rb[j : j + PADW, :].astype(BF16)


def conv(src, wref, starts, rows, width, flip):
    C, acc = wref.shape[3], None
    for i in range(3):
        for j in range(3):
            parts = [src[j, b + i : b + i + rows, 0:width, :].reshape(rows * width, C) for b in starts]
            lhs = parts[0] if len(parts) == 1 else jnp.concatenate(parts)
            w = wref[2 - i, 2 - j] if flip else wref[i, j]
            dims = (((1,), (1 if flip else 0,)), ((), ()))
            t = lax.dot_general(lhs, w, dims, preferred_element_type=F32)
            acc = t if acc is None else acc + t
    return acc


def inner_rows(c1, c2, r, half_two, bias_two, cmask):
    cut = slice(r * PADW, (r + 1) * PADW)
    return c2[cut] * half_two * slope_of(c1[cut] * half_two + bias_two) * cmask


def store_inner(rb, g, dst, h, W):
    rb[0:PADW, :] = g
    for j in range(3):
        dst[j, h, :, :] = rb[j : j + W, :].astype(BF16)


def col_mask(to_left, to_right, W):
    pos = lax.broadcasted_iota(jnp.int32, (PADW, 1), 0)
    return jnp.where(pos == 0, to_left, jnp.where(pos == W + 1, to_right, 1.0))


def result_row(x, g, c3, half_one, bias_one):
    v = x.astype(F32) * half_one + bias_one
    return (g.astype(F32) + c3 * half_one * slope_of(v)).astype(BF16)


def middle_kernel(
    stats, vecs, img, cot, ce, co, k1, w2, out, kept, rowbuf, act3, cot3, in3, res, nbuf, fbuf, k2, sems
):
    H, W, C = img.shape[1:]
    load = pltpu.make_async_copy(w2, k2, sems.at[0])
    load.start()
    half_one, bias_one, half_two, bias_two = affine(stats, vecs, C)
    odd_row, odd_col, (up, down, to_left, to_right) = place()
    for k in range(2):
        nbuf[k], fbuf[k] = ce[k].astype(F32), co[k].astype(F32)

    def prepare(rows):
        for h in rows:
            for k, (src, dst) in enumerate(((img, act3), (cot, cot3))):
                cut = slice(2 * h, 2 * h + 2)
                near, far = nbuf[k, cut], fbuf[k, cut]
                lft, rgt = jnp.where(odd_col, near, far), jnp.where(odd_col, far, near)
                own = src[0, h]
                if k == 0:
                    own = act_of(own, half_one, bias_one)
                    lft, rgt = act_of(lft, half_one, bias_one) * to_left, act_of(rgt, half_one, bias_one) * to_right
                fill(rowbuf.at[(2 * h + k) % 4], own, lft, rgt, dst, h)

    cmask = col_mask(to_left, to_right, W)
    R = (H - 2) // 2
    prepare(range(R + 2))
    load.wait()
    for b in range(0, H - 2, R):
        c1 = conv(act3, k1, (b,), R, PADW, False)
        if b == 0:
            prepare(range(R + 2, H))
        c2 = conv(cot3, k2, (b,), R, PADW, True)
        for r in range(R):
            g = inner_rows(c1, c2, r, half_two, bias_two, cmask)
            store_inner(rowbuf.at[4 + r % 4], g, in3, b + r, W)
    for j in range(3):
        for s, h in enumerate((0, 1, H - 4, H - 3)):
            kept[j, s] = in3[j, h]
    R = (H - 4) // 2
    stores = []
    for b in range(0, H - 4, R):
        c3 = conv(in3, k1, (b,), R, W, True)
        for r in range(R):
            h = b + r + 2
            res[b + r] = result_row(img[0, h], cot[0, h], c3[r * W : (r + 1) * W], half_one, bias_one)
        stores.append(pltpu.make_async_copy(res.at[b : b + R], out.at[0, b + 2 : b + 2 + R], sems.at[2 + b // R]))
        stores[-1].start()
    for store in stores:
        store.wait()


def middle(stats, vecs, img, cot, ce, co, k1, k2):
    H, W, C = img.shape[1:]
    return pl.pallas_call(
        middle_kernel,
        out_shape=(jax.ShapeDtypeStruct(img.shape, BF16), jax.ShapeDtypeStruct((3, 4, W, C), BF16)),
        in_specs=[(SMEM,) * 4, (VMEM,) * 5] + [VMEM] * 5 + [HBM],
        out_specs=(HBM, VMEM),
        scratch_shapes=[
            pltpu.VMEM((8, PADW + 16, C), F32),
            pltpu.VMEM((3, H, PADW, C), BF16),
            pltpu.VMEM((3, H, PADW, C), BF16),
            pltpu.VMEM((3, H - 2, W, C), BF16),
            pltpu.VMEM((H - 4, W, C), BF16),
            pltpu.VMEM((2, 2 * H, C), F32),
            pltpu.VMEM((2, 2 * H, C), F32),
            pltpu.VMEM(k2.shape, BF16),
            pltpu.SemaphoreType.DMA((4,)),
        ],
        compiler_params=LARGE,
        name="middle",
    )(stats, vecs, img, cot, ce, co, k1, k2)


def border_kernel(
    stats, vecs, img, cot, ce, co, odd, even, k1, w2, kept, old, out,
    rowbuf, act3, cot3, in3, res, nbuf, fbuf, k2, sems,
):
    H, W, C = img.shape[1:]
    m = 2 * H
    load = pltpu.make_async_copy(w2, k2, sems.at[0])
    load.start()
    half_one, bias_one, half_two, bias_two = affine(stats, vecs, C)
    odd_row, odd_col, (up, down, to_left, to_right) = place()
    for k in range(2):
        nbuf[k, 4 : m + 4], fbuf[k, 4 : m + 4] = ce[k].astype(F32), co[k].astype(F32)
        o, e = odd[k, 2 * W : 2 * W + 16].astype(F32), even[k, 2 * W : 2 * W + 16].astype(F32)
        near_odd, near_even, far_odd, far_even = o[0:4], e[0:4], o[4:8], e[4:8]
        nbuf[k, 0:4] = jnp.where(odd_row, near_even, near_odd)
        nbuf[k, m + 4 : m + 8] = jnp.where(odd_row, near_odd, near_even)
        fbuf[k, 0:4] = jnp.where(odd_row, far_even, far_odd)
        fbuf[k, m + 4 : m + 8] = jnp.where(odd_row, far_odd, far_even)
    count = 0
    for s, h in enumerate((0, 1, 2, 3, H, H + 1, H + 2, H + 3)):
        for k, (src, dst) in enumerate(((img, act3), (cot, cot3))):
            mask = None
            if h < 2 or h >= H + 2:
                t = h if h < 2 else h - H - 2
                cut = slice(t * W, (t + 1) * W)
                o, e = odd[k, cut], even[k, cut]
                own = jnp.where(odd_row, e, o) if h < 2 else jnp.where(odd_row, o, e)
                mask = up if h < 2 else down
            else:
                own = src[0, h - 2]
            near, far = nbuf[k, 2 * h : 2 * h + 2], fbuf[k, 2 * h : 2 * h + 2]
            lft, rgt = jnp.where(odd_col, near, far), jnp.where(odd_col, far, near)
            if k == 0:
                own = act_of(own, half_one, bias_one)
                lft, rgt = act_of(lft, half_one, bias_one) * to_left, act_of(rgt, half_one, bias_one) * to_right
                if mask is not None:
                    own, lft, rgt = own * mask, lft * mask, rgt * mask
            fill(rowbuf.at[count % 4], own, lft, rgt, dst, s)
            count += 1
    for j in range(3):
        for s, d in enumerate((2, 3, 4, 5)):
            in3[j, d] = kept[j, s]
    load.wait()
    cmask = col_mask(to_left, to_right, W)
    c1 = conv(act3, k1, (0, 4), 2, PADW, False)
    c2 = conv(cot3, k2, (0, 4), 2, PADW, True)
    for r, (d, mask) in enumerate(((0, up), (1, None), (6, None), (7, down))):
        g = inner_rows(c1, c2, r, half_two, bias_two, cmask)
        store_inner(rowbuf.at[r], g if mask is None else g * mask, in3, d, W)
    c3 = conv(in3, k1, (0, 4), 2, W, True)
    for r, h in enumerate((0, 1, H - 2, H - 1)):
        res[r] = result_row(img[0, h], cot[0, h], c3[r * W : (r + 1) * W], half_one, bias_one)
    stores = [
        pltpu.make_async_copy(res.at[0:2], out.at[0, 0:2], sems.at[2]),
        pltpu.make_async_copy(res.at[2:4], out.at[0, H - 2 : H], sems.at[3]),
    ]
    for store in stores:
        store.start()
    for store in stores:
        store.wait()


def border(stats, vecs, img, cot, ce, co, odd, even, k1, k2, kept, old):
    H, W, C = img.shape[1:]
    return pl.pallas_call(
        border_kernel,
        out_shape=jax.ShapeDtypeStruct(img.shape, BF16),
        in_specs=[(SMEM,) * 4, (VMEM,) * 5] + [VMEM] * 7 + [HBM, VMEM, HBM],
        out_specs=HBM,
        input_output_aliases={4 + 5 + 6 + 3: 0},
        scratch_shapes=[
            pltpu.VMEM((4, PADW + 16, C), F32),
            pltpu.VMEM((3, 8, PADW, C), BF16),
            pltpu.VMEM((3, 8, PADW, C), BF16),
            pltpu.VMEM((3, 8, W, C), BF16),
            pltpu.VMEM((4, W, C), BF16),
            pltpu.VMEM((2, 2 * H + 8, C), F32),
            pltpu.VMEM((2, 2 * H + 8, C), F32),
            pltpu.VMEM(k2.shape, BF16),
            pltpu.SemaphoreType.DMA((4,)),
        ],
        compiler_params=LARGE,
        name="border",
    )(stats, vecs, img, cot, ce, co, odd, even, k1, k2, kept, old)


def swaps(size, first):
    return [pair for i in range(first, size - 1, 2) for pair in ((i, i + 1), (i + 1, i))]


def per_device(
    image_in,
    cotangent,
    first_kernel,
    first_bias,
    second_kernel,
    first_center,
    first_inverse,
    first_gain,
    first_shift,
    second_center,
    second_inverse,
    second_gain,
    second_shift,
):
    stats = (first_center, first_inverse, second_center, second_inverse)
    vecs = tuple(v[None] for v in (first_bias, first_gain, first_shift, second_gain, second_shift))

    def send(name, x):
        axis = COLS if name[0] == "c" else ROWS
        return lax.ppermute(x, axis, swaps(lax.axis_size(axis), int(name[1] == "o")))

    stay = lambda x: pltpu.with_memory_space_constraint(x, pltpu.HBM)
    second_kernel = stay(second_kernel)
    near, far = edges(stay(image_in), stay(cotangent))
    co, ce = send("co", far), send("ce", near)
    odd, even = messages(image_in, cotangent, ce, co)
    odd, even = send("ro", odd), send("re", even)
    out, kept = middle(stats, vecs, image_in, cotangent, ce, co, first_kernel, second_kernel)
    return border(stats, vecs, image_in, cotangent, ce, co, odd, even, first_kernel, second_kernel, kept, out)


def solution(mesh):
    tiled, whole = P(None, ROWS, COLS, None), P()
    return jax.shard_map(
        per_device,
        mesh=mesh,
        in_specs=(tiled, tiled) + (whole,) * 11,
        out_specs=tiled,
        check_vma=False,
    )
```
